16 devices in a mesh: data: 2 (over y, z), model: 8 (over x, core).
Axes of the slice: x: 4, y: 2, z: 1, core: 2. Of those that a mesh axis runs over, the one named last changes fastest.
The devices are a block of a 4x4x8 slice.
Arguments:
- x_in: bfloat16 [2, 4096, 3072], P('data'), parts along dimension 0
- seg_ids: int32 [2, 4096], P('data'), parts along dimension 0
- gain_one: bfloat16 [3072], replicated
- w_qkv: bfloat16 [3072, 9216], P(None, 'model')
- w_out: bfloat16 [32, 96, 3072], P('model')
- gain_two: bfloat16 [3072], replicated
- w_up: bfloat16 [3072, 12288], P(None, 'model')
- w_down: bfloat16 [12288, 3072], P('model')
- d_y: bfloat16 [2, 4096, 3072], P('data'), parts along dimension 0
Outputs:
- output 1: bfloat16 [2, 4096, 3072], P('data'), parts along dimension 0
- output 2: bfloat16 [2, 4096, 3072], P('data'), parts along dimension 0
- output 3: bfloat16 [6144, 9216], P('data', 'model'), parts along dimension 0
- output 4: bfloat16 [64, 96, 3072], P(('data', 'model')), parts along dimension 0
- output 5: bfloat16 [6144, 12288], P('data', 'model'), parts along dimension 0
- output 6: bfloat16 [24576, 3072], P(('data', 'model')), parts along dimension 0
- output 7: bfloat16 [6144], P('data'), parts along dimension 0
- output 8: bfloat16 [6144], P('data'), parts along dimension 0
There are 2 independent parts. The reference program is written for one: setup_inputs(seed, part) draws one part's arguments, and reference() takes and returns one part's arrays. A program takes and returns all parts, laid end to end along the dimension named above; an argument that names none is the same for every part.
All inputs are finite; a program needn't handle non-finite values.
Results may differ from the reference program's by a relative error of at most 0.02.
Values are sent between devices in bfloat16 or wider.
A program may use at most 768 MiB of HBM per device.

```python
import jax
import jax.numpy as jnp
from jax import lax

BATCH_ROWS = 1
SEQ_LEN = 4096
MODEL_DIM = 3072
NUM_HEADS = 32
HEAD_DIM = 96
FFN_DIM = 12288
LN_EPS = 1e-5
TOKEN_COUNT = BATCH_ROWS * SEQ_LEN
QKV_WIDTH = 3 * NUM_HEADS * HEAD_DIM
INNER_WIDTH = NUM_HEADS * HEAD_DIM


def draw_segments(seg_key):
    seg_keys = jax.random.split(seg_key, 3)
    rate_table = jnp.array([0, 2, 8, 32], jnp.int32)
    row_rate = rate_table[jax.random.randint(seg_keys[0], (BATCH_ROWS,), 0, 4)]
    pos_draws = jax.random.randint(seg_keys[1], (BATCH_ROWS, SEQ_LEN), 0, SEQ_LEN)
    forced_pos = jax.random.randint(seg_keys[2], (BATCH_ROWS,), 1, SEQ_LEN)
    positions = jnp.arange(SEQ_LEN, dtype=jnp.int32)
    breaks = ((pos_draws < row_rate[:, None]) | (positions[None, :] == forced_pos[:, None])).astype(jnp.int32)
    breaks = breaks.at[:, 0].set(0)
    return jnp.cumsum(breaks, axis=1).astype(jnp.int32)


def setup_inputs(seed: int = 0, part: int = 0) -> dict:
    base_key = jax.random.key(seed)
    part_key = jax.random.fold_in(base_key, part)
    weight_keys = jax.random.split(base_key, 6)
    part_keys = jax.random.split(part_key, 4)
    x_in = jax.random.normal(part_keys[0], (BATCH_ROWS, SEQ_LEN, MODEL_DIM), jnp.float32)
    seg_ids = draw_segments(part_keys[1])
    gain_one = 1.0 + 0.3 * jax.random.normal(weight_keys[0], (MODEL_DIM,), jnp.float32)
    gain_two = 1.0 + 0.3 * jax.random.normal(weight_keys[1], (MODEL_DIM,), jnp.float32)
    w_qkv = jax.random.normal(weight_keys[2], (MODEL_DIM, QKV_WIDTH), jnp.float32) * (1.5 * MODEL_DIM ** -0.5)
    w_out = jax.random.normal(weight_keys[3], (NUM_HEADS, HEAD_DIM, MODEL_DIM), jnp.float32) * INNER_WIDTH ** -0.5
    w_up = jax.random.normal(weight_keys[4], (MODEL_DIM, FFN_DIM), jnp.float32) * MODEL_DIM ** -0.5
    w_down = jax.random.normal(weight_keys[5], (FFN_DIM, MODEL_DIM), jnp.float32) * FFN_DIM ** -0.5
    d_y = jax.random.normal(part_keys[3], (BATCH_ROWS, SEQ_LEN, MODEL_DIM), jnp.float32)
    return {'x_in': x_in.astype(jnp.bfloat16), 'seg_ids': seg_ids, 'gain_one': gain_one.astype(jnp.bfloat16), 'w_qkv': w_qkv.astype(jnp.bfloat16), 'w_out': w_out.astype(jnp.bfloat16), 'gain_two': gain_two.astype(jnp.bfloat16), 'w_up': w_up.astype(jnp.bfloat16), 'w_down': w_down.astype(jnp.bfloat16), 'd_y': d_y.astype(jnp.bfloat16)}


def layer_norm(x_in, gain):
    x_wide = x_in.astype(jnp.float32)
    row_mean = jnp.mean(x_wide, axis=-1, keepdims=True)
    centered = x_wide - row_mean
    row_var = jnp.mean(centered * centered, axis=-1, keepdims=True)
    return (centered * lax.rsqrt(row_var + LN_EPS) * gain.astype(jnp.float32)).astype(jnp.bfloat16)


def head_attention(q_head, k_head, v_head, seg_ids):
    positions = jnp.arange(SEQ_LEN)
    allowed = (positions[:, None] >= positions[None, :])[None] & (seg_ids[:, :, None] == seg_ids[:, None, :])
    scores = jnp.einsum('bqd,bkd->bqk', q_head.astype(jnp.float32), k_head.astype(jnp.float32)) * (HEAD_DIM ** -0.5)
    scores = jnp.where(allowed, scores, -1e30)
    attn_prob = jax.nn.softmax(scores, axis=-1).astype(jnp.bfloat16)
    result = jnp.einsum('bqk,bkd->bqd', attn_prob.astype(jnp.float32), v_head.astype(jnp.float32))
    return result.astype(jnp.bfloat16)


def layer_forward(x_in, seg_ids, gain_one, w_qkv, w_out, gain_two, w_up, w_down):
    x_flat = x_in.reshape(TOKEN_COUNT, MODEL_DIM)
    normed_one = layer_norm(x_flat, gain_one)
    qkv_proj = jnp.dot(normed_one, w_qkv, preferred_element_type=jnp.float32).astype(jnp.bfloat16)
    qkv_heads = jnp.moveaxis(qkv_proj.reshape(BATCH_ROWS, SEQ_LEN, NUM_HEADS, 3, HEAD_DIM), 2, 0)

    def one_head(head_qkv):
        return head_attention(head_qkv[:, :, 0], head_qkv[:, :, 1], head_qkv[:, :, 2], seg_ids)

    attn_heads = lax.map(jax.checkpoint(one_head), qkv_heads)
    attn_flat = jnp.moveaxis(attn_heads, 0, 2).reshape(TOKEN_COUNT, INNER_WIDTH)
    proj_one = jnp.dot(attn_flat, w_out.reshape(INNER_WIDTH, MODEL_DIM), preferred_element_type=jnp.float32)
    resid = (x_flat.astype(jnp.float32) + proj_one).astype(jnp.bfloat16)
    normed_two = layer_norm(resid, gain_two)
    up_proj = jnp.dot(normed_two, w_up, preferred_element_type=jnp.float32).astype(jnp.bfloat16)
    gelu_out = jax.nn.gelu(up_proj.astype(jnp.float32), approximate=True).astype(jnp.bfloat16)
    proj_two = jnp.dot(gelu_out, w_down, preferred_element_type=jnp.float32)
    y_flat = (resid.astype(jnp.float32) + proj_two).astype(jnp.bfloat16)
    return y_flat.reshape(BATCH_ROWS, SEQ_LEN, MODEL_DIM)


def reference(x_in, seg_ids, gain_one, w_qkv, w_out, gain_two, w_up, w_down, d_y):
    def forward_fn(x_arg, g_one, wq_arg, wo_arg, g_two, wu_arg, wd_arg):
        return layer_forward(x_arg, seg_ids, g_one, wq_arg, wo_arg, g_two, wu_arg, wd_arg)

    y_out, pullback = jax.vjp(forward_fn, x_in, gain_one, w_qkv, w_out, gain_two, w_up, w_down)
    d_x, d_gain_one, d_w_qkv, d_w_out, d_gain_two, d_w_up, d_w_down = pullback(d_y)
    return (y_out, d_x, d_w_qkv, d_w_out, d_w_up, d_w_down, d_gain_one, d_gain_two)
```

```python
import functools

import jax
import jax.numpy as jnp
from jax import lax
from jax.experimental import pallas as pl
from jax.experimental.pallas import tpu as pltpu
from jax.sharding import PartitionSpec as P

LN_EPS = 1e-5
LOG2E = 1.4426950408889634
MASKED = -1e30
N_CHUNKS = 2
VMEM_BYTES = 60 * 1024 * 1024
NT = (((1,), (1,)), ((), ()))
TN = (((0,), (0,)), ((), ()))
F32, BF16 = jnp.float32, jnp.bfloat16


def mm(a, b, dims):
    return lax.dot_general(a, b, (dims, ((), ())), preferred_element_type=F32)


def layer_norm(x_in, gain):
    x_wide = x_in.astype(F32)
    row_mean = jnp.mean(x_wide, axis=-1, keepdims=True)
    centered = x_wide - row_mean
    row_var = jnp.mean(centered * centered, axis=-1, keepdims=True)
    return (centered * lax.rsqrt(row_var + LN_EPS) * gain.astype(F32)).astype(BF16)


def gelu_tanh(up_proj):
    return jax.nn.gelu(up_proj.astype(F32), approximate=True).astype(BF16)


def after(value, *others):
    return lax.optimization_barrier((value, *others))[0]


def document_starts(seg):
    seq = seg.shape[0]
    side = 64
    before = jnp.concatenate([seg[:1], seg[:-1]])
    marks = jnp.where(seg != before, jnp.arange(seq, dtype=jnp.int32), 0).reshape(seq // side, side)
    upto = jnp.arange(side)[:, None] >= jnp.arange(side)[None, :]
    inside = jnp.max(jnp.where(upto[None], marks[:, None, :], 0), axis=-1)
    row = jnp.arange(seq // side)
    ahead = jnp.max(jnp.where(row[:, None] > row[None, :], jnp.max(marks, axis=-1)[None, :], 0), axis=-1)
    return jnp.maximum(inside, ahead[:, None]).reshape(seq)


def ln_qkv_kernel(x_ref, g_ref, w_ref, a_ref, qkv_ref):
    normed = layer_norm(x_ref[...], g_ref[...])
    a_ref[...] = normed
    qkv_ref[...] = jnp.dot(normed, w_ref[...], preferred_element_type=F32).astype(BF16)


def ln_qkv(x, gain, w, rows=256):
    t, h = x.shape
    c = w.shape[1]
    return pl.pallas_call(
        ln_qkv_kernel,
        grid=(t // rows,),
        in_specs=[
            pl.BlockSpec((rows, h), lambda i: (i, 0)),
            pl.BlockSpec((1, h), lambda i: (0, 0)),
            pl.BlockSpec((h, c), lambda i: (0, 0)),
        ],
        out_specs=[pl.BlockSpec((rows, h), lambda i: (i, 0)), pl.BlockSpec((rows, c), lambda i: (i, 0))],
        out_shape=[jax.ShapeDtypeStruct((t, h), BF16), jax.ShapeDtypeStruct((t, c), BF16)],
        compiler_params=pltpu.CompilerParams(vmem_limit_bytes=VMEM_BYTES, dimension_semantics=('arbitrary',)),
        cost_estimate=pl.CostEstimate(flops=2 * t * h * c, bytes_accessed=4 * t * h + 2 * h * c + 2 * t * c, transcendentals=0),
        name='ln_qkv',
    )(x, gain.reshape(1, h), w)


def proj_ln_kernel(o_ref, w_ref, x_ref, g_ref, resid_ref, b_ref):
    acc = x_ref[...].astype(F32)
    for r in range(o_ref.shape[0]):
        acc = acc + jnp.dot(o_ref[r], w_ref[r], preferred_element_type=F32)
    resid = acc.astype(BF16)
    resid_ref[...] = resid
    b_ref[...] = layer_norm(resid, g_ref[...])


def proj_ln(o_all, w_all, x, gain, row0, rows=256):
    n, t, d = o_all.shape
    h = x.shape[1]
    first = row0 // rows
    return pl.pallas_call(
        proj_ln_kernel,
        grid=(t // rows,),
        in_specs=[
            pl.BlockSpec((n, rows, d), lambda i: (0, i, 0)),
            pl.BlockSpec((n, d, h), lambda i: (0, 0, 0), pipeline_mode=pl.Buffered(1)),
            pl.BlockSpec((rows, h), lambda i: (i + first, 0)),
            pl.BlockSpec((1, h), lambda i: (0, 0)),
        ],
        out_specs=[pl.BlockSpec((rows, h), lambda i: (i, 0))] * 2,
        out_shape=[jax.ShapeDtypeStruct((t, h), BF16)] * 2,
        compiler_params=pltpu.CompilerParams(vmem_limit_bytes=VMEM_BYTES, dimension_semantics=('arbitrary',)),
        cost_estimate=pl.CostEstimate(flops=2 * t * n * d * h, bytes_accessed=2 * n * d * h + 8 * t * h, transcendentals=0),
        name='proj_ln',
    )(o_all, w_all, x, gain.reshape(1, h))


def place_kernel(part_ref, *refs):
    refs[-1][...] = part_ref[...]


def place(part, into, seq, row0, rows=256):
    t, h = part.shape
    first = row0 // rows
    in_specs = [pl.BlockSpec((rows, h), lambda i: (i, 0))]
    if into is not None:
        in_specs.append(pl.BlockSpec(memory_space=pl.ANY))
    return pl.pallas_call(
        place_kernel,
        grid=(t // rows,),
        in_specs=in_specs,
        out_specs=pl.BlockSpec((rows, h), lambda i: (i + first, 0)),
        out_shape=jax.ShapeDtypeStruct((seq, h), part.dtype),
        input_output_aliases={} if into is None else {1: 0},
        compiler_params=pltpu.CompilerParams(vmem_limit_bytes=16 * 1024 * 1024, dimension_semantics=('arbitrary',)),
        cost_estimate=pl.CostEstimate(flops=16 * t * h, bytes_accessed=4 * t * h, transcendentals=0),
        name='place',
    )(part, *(() if into is None else (into,)))


def split_kv(qkv_ref, k_scr, v_scr, blk):
    n, rows, d = k_scr.shape

    def body(j, carry):
        at = pl.ds(pl.multiple_of(j * blk, blk), blk)
        for h in range(n):
            k_scr[h, at, :] = qkv_ref[at, (3 * h + 1) * d:(3 * h + 2) * d]
            v_scr[h, at, :] = qkv_ref[at, (3 * h + 2) * d:(3 * h + 3) * d]
        return carry

    lax.fori_loop(0, rows // blk, body, 0)


def attn_fwd_kernel(first, low_ref, mid_ref, q_ref, kv_ref, start_ref, o_ref, lse_ref, k_scr, v_scr, m_scr, l_scr, acc_scr):
    step = pl.program_id(0)
    n, _, d = k_scr.shape
    blk = q_ref.shape[0]
    scale = d ** -0.5 * LOG2E

    @pl.when(step == 0)
    def _():
        split_kv(kv_ref, k_scr, v_scr, blk)

    i = step + first
    queries = [q_ref[:, 3 * h * d:(3 * h + 1) * d] for h in range(n)]
    start = start_ref[...]
    m_scr[...] = jnp.full(m_scr.shape, MASKED, F32)
    l_scr[...] = jnp.zeros(l_scr.shape, F32)
    acc_scr[...] = jnp.zeros(acc_scr.shape, F32)

    def block(j, kind):
        at = pl.ds(pl.multiple_of(j * blk, blk), blk)
        if kind != 'full':
            cols = j * blk + lax.broadcasted_iota(jnp.int32, (blk, blk), 1)
            seen = cols >= start
            if kind == 'diagonal':
                seen = seen & (cols <= i * blk + lax.broadcasted_iota(jnp.int32, (blk, blk), 0))
        for h in range(n):
            s = lax.dot_general(queries[h], k_scr[h, at, :], NT, preferred_element_type=F32) * scale
            if kind != 'full':
                s = jnp.where(seen, s, MASKED)
            m_old = m_scr[h]
            m_new = jnp.maximum(m_old, jnp.max(s, axis=-1, keepdims=True))
            p = jnp.exp2(s - m_new)
            alpha = jnp.exp2(m_old - m_new)
            l_scr[h] = l_scr[h] * alpha + jnp.sum(p, axis=-1, keepdims=True)
            m_scr[h] = m_new
            acc_scr[h] = acc_scr[h] * alpha + jnp.dot(p.astype(BF16), v_scr[h, at, :], preferred_element_type=F32)

    low = low_ref[i]
    mid = jnp.minimum(mid_ref[i], i)
    pl.loop(low, mid)(lambda j: block(j, 'masked'))
    pl.loop(mid, i)(lambda j: block(j, 'full'))
    block(i, 'diagonal')
    lanes = lax.broadcasted_iota(jnp.int32, lse_ref.shape, 1)
    lse = jnp.zeros(lse_ref.shape, F32)
    for h in range(n):
        total = l_scr[h]
        o_ref[:, h * d:(h + 1) * d] = (acc_scr[h] / total).astype(BF16)
        lse = jnp.where(lanes == h, m_scr[h] + jnp.log2(total), lse)
    lse_ref[...] = lse


def attn_fwd(qkv, start, low, mid, n, d, row0, row1, blk):
    rows = row1 - row0
    c = qkv.shape[1]
    first = row0 // blk
    pairs = n * (row1 * row1 - row0 * row0) // 2
    return pl.pallas_call(
        functools.partial(attn_fwd_kernel, first),
        grid_spec=pltpu.PrefetchScalarGridSpec(
            num_scalar_prefetch=2,
            grid=(rows // blk,),
            in_specs=[
                pl.BlockSpec((blk, c), lambda i, *_: (i + first, 0)),
                pl.BlockSpec((row1, c), lambda i, *_: (0, 0), pipeline_mode=pl.Buffered(1)),
                pl.BlockSpec((blk, 1), lambda i, *_: (i + first, 0)),
            ],
            out_specs=[pl.BlockSpec((blk, n * d), lambda i, *_: (i, 0)), pl.BlockSpec((blk, 128), lambda i, *_: (i, 0))],
            scratch_shapes=[
                pltpu.VMEM((n, row1, d), BF16),
                pltpu.VMEM((n, row1, d), BF16),
                pltpu.VMEM((n, blk, 1), F32),
                pltpu.VMEM((n, blk, 1), F32),
                pltpu.VMEM((n, blk, d), F32),
            ],
        ),
        out_shape=[jax.ShapeDtypeStruct((rows, n * d), BF16), jax.ShapeDtypeStruct((rows, 128), F32)],
        compiler_params=pltpu.CompilerParams(vmem_limit_bytes=VMEM_BYTES, dimension_semantics=('arbitrary',)),
        cost_estimate=pl.CostEstimate(flops=2 * 4 * pairs * d, bytes_accessed=2 * row1 * c + 2 * rows * n * d, transcendentals=pairs),
        name='attn_fwd',
    )(low, mid, qkv, qkv, start)


def attn_bwd_kernel(last, final, low_ref, mid_ref, q_ref, kv_ref, start_ref, do_ref, o_ref, lse_ref, *rest):
    if final:
        carry_ref, out_ref, k_scr, v_scr, acc_scr, dq_scr, stat_scr, sem = rest
    else:
        out_ref, carry_ref, k_scr, v_scr, acc_scr, dq_scr, stat_scr, sem = rest
    step = pl.program_id(0)
    n, _, d = k_scr.shape
    blk = q_ref.shape[0]
    scale = d ** -0.5

    @pl.when(step == 0)
    def _():
        split_kv(kv_ref, k_scr, v_scr, blk)
        if final:
            copy = pltpu.make_async_copy(carry_ref, acc_scr, sem)
            copy.start()
            copy.wait()
        else:
            def clear(j, carry):
                at = pl.ds(pl.multiple_of(j * blk, blk), blk)
                for h in range(2 * n):
                    acc_scr[h, at, :] = jnp.zeros((blk, d), F32)
                return carry
            lax.fori_loop(0, acc_scr.shape[1] // blk, clear, 0)

    i = last - step
    queries = [q_ref[:, 3 * h * d:(3 * h + 1) * d] for h in range(n)]
    d_outs = [do_ref[:, h * d:(h + 1) * d] for h in range(n)]
    start = start_ref[...]
    lanes = lax.broadcasted_iota(jnp.int32, lse_ref.shape, 1)
    delta = jnp.zeros(lse_ref.shape, F32)
    for h in range(n):
        prod = d_outs[h].astype(F32) * o_ref[:, h * d:(h + 1) * d].astype(F32)
        delta = jnp.where(lanes == h, jnp.sum(prod, axis=-1, keepdims=True), delta)
    stat_scr[0] = jnp.transpose(lse_ref[...])[:8]
    stat_scr[1] = jnp.transpose(delta)[:8]
    dq_scr[...] = jnp.zeros(dq_scr.shape, F32)

    def block(j, kind):
        at = pl.ds(pl.multiple_of(j * blk, blk), blk)
        if kind != 'full':
            keys = j * blk + lax.broadcasted_iota(jnp.int32, (blk, blk), 0)
            seen = keys >= start
            if kind == 'diagonal':
                seen = seen & (keys <= i * blk + lax.broadcasted_iota(jnp.int32, (blk, blk), 1))
        for h in range(n):
            k = k_scr[h, at, :]
            s = lax.dot_general(k, queries[h], NT, preferred_element_type=F32) * (scale * LOG2E)
            if kind != 'full':
                s = jnp.where(seen, s, MASKED)
            p = jnp.exp2(s - stat_scr[0, h:h + 1, :])
            dp = lax.dot_general(v_scr[h, at, :], d_outs[h], NT, preferred_element_type=F32)
            ds = (p * (dp - stat_scr[1, h:h + 1, :])).astype(BF16)
            acc_scr[n + h, at, :] += jnp.dot(p.astype(BF16), d_outs[h], preferred_element_type=F32)
            acc_scr[h, at, :] += jnp.dot(ds, queries[h], preferred_element_type=F32)
            dq_scr[h] += lax.dot_general(ds, k, TN, preferred_element_type=F32)

    low = low_ref[i]
    mid = jnp.minimum(mid_ref[i], i)
    pl.loop(low, mid)(lambda j: block(j, 'masked'))
    pl.loop(mid, i)(lambda j: block(j, 'full'))
    block(i, 'diagonal')
    at = pl.ds(pl.multiple_of(i * blk, blk), blk)
    for h in range(n):
        out_ref[:, 3 * h * d:(3 * h + 1) * d] = (dq_scr[h] * scale).astype(BF16)
        out_ref[:, (3 * h + 1) * d:(3 * h + 2) * d] = (acc_scr[h, at, :] * scale).astype(BF16)
        out_ref[:, (3 * h + 2) * d:(3 * h + 3) * d] = acc_scr[n + h, at, :].astype(BF16)

    if not final:
        @pl.when(step == pl.num_programs(0) - 1)
        def _():
            copy = pltpu.make_async_copy(acc_scr.at[:, 0:carry_ref.shape[1], :], carry_ref, sem)
            copy.start()
            copy.wait()


def attn_bwd(qkv, start_row, low, mid, d_out, o, lse, carry, n, d, row0, row1, blk):
    rows = row1 - row0
    c = qkv.shape[1]
    count = rows // blk
    last = row1 // blk - 1
    final = row0 == 0
    pairs = n * (row1 * row1 - row0 * row0) // 2
    out_shape = [jax.ShapeDtypeStruct((rows, c), BF16)]
    out_specs = [pl.BlockSpec((blk, c), lambda i, *_: (count - 1 - i, 0))]
    in_specs = [
        pl.BlockSpec((blk, c), lambda i, *_: (last - i, 0)),
        pl.BlockSpec((row1, c), lambda i, *_: (0, 0), pipeline_mode=pl.Buffered(1)),
        pl.BlockSpec((1, blk), lambda i, *_: (0, last - i)),
        pl.BlockSpec((blk, n * d), lambda i, *_: (count - 1 - i, 0)),
        pl.BlockSpec((blk, n * d), lambda i, *_: (count - 1 - i, 0)),
        pl.BlockSpec((blk, 128), lambda i, *_: (count - 1 - i, 0)),
    ]
    args = [low, mid, qkv, qkv, start_row, d_out, o, lse]
    assert final == (carry is not None) or row1 == qkv.shape[0]
    if final:
        if carry is None:
            carry = jnp.zeros((2 * n, row1, d), F32)
        in_specs.append(pl.BlockSpec(memory_space=pl.ANY))
        args.append(carry)
    else:
        out_shape.append(jax.ShapeDtypeStruct((2 * n, row0, d), F32))
        out_specs.append(pl.BlockSpec(memory_space=pl.ANY))
    return pl.pallas_call(
        functools.partial(attn_bwd_kernel, last, final),
        grid_spec=pltpu.PrefetchScalarGridSpec(
            num_scalar_prefetch=2,
            grid=(count,),
            in_specs=in_specs,
            out_specs=out_specs,
            scratch_shapes=[
                pltpu.VMEM((n, row1, d), BF16),
                pltpu.VMEM((n, row1, d), BF16),
                pltpu.VMEM((2 * n, row1, d), F32),
                pltpu.VMEM((n, blk, d), F32),
                pltpu.VMEM((2, 8, blk), F32),
                pltpu.SemaphoreType.DMA,
            ],
        ),
        out_shape=out_shape,
        compiler_params=pltpu.CompilerParams(vmem_limit_bytes=VMEM_BYTES, dimension_semantics=('arbitrary',)),
        cost_estimate=pl.CostEstimate(flops=2 * 10 * pairs * d, bytes_accessed=4 * row1 * c + 4 * rows * n * d, transcendentals=pairs),
        name='attn_bwd',
    )(*args)


def solution(mesh):
    def local_step(x_in, seg_ids, gain_one, w_qkv, w_out, gain_two, w_up, w_down, d_y):
        rows, seq, hidden = x_in.shape
        n, d = w_out.shape[:2]
        blk = min(512, seq)
        size = seq // N_CHUNKS
        order = [(c * size, (c + 1) * size) for c in range(N_CHUNKS)][::-1]
        me = lax.axis_index('model')
        share = size // mesh.shape['model']

        def mine(full, row0):
            return lax.dynamic_slice_in_dim(full, row0 + me * share, share, 0)

        def gather(part):
            return lax.all_gather(part, 'model', axis=0, tiled=True)

        def scatter(part):
            return lax.psum_scatter(part, 'model', scatter_dimension=0, tiled=True)

        outs = []
        for b in range(rows):
            x, dy, seg = x_in[b], d_y[b], seg_ids[b]
            start = document_starts(seg)
            low = start[::blk] // blk
            mid = (start[blk - 1::blk] + blk - 1) // blk
            start_col, start_row = start.reshape(seq, 1), start.reshape(1, seq)

            wo = w_out.reshape(n * d, hidden)
            wo_all = gather(wo).reshape(-1, n * d, hidden)
            normed_one, qkv = ln_qkv(x, gain_one, w_qkv)
            attn, lse, attn_all = {}, {}, {}
            prev = ()
            for row0, row1 in order:
                attn[row0], lse[row0] = attn_fwd(after(qkv, *prev), start_col, low, mid, n, d, row0, row1, blk)
                attn_all[row0] = lax.all_gather(attn[row0], 'model', axis=0, tiled=False)
                prev = (attn[row0], wo_all)
            d_gelu = mm(after(dy, *prev), w_down, ((1,), (1,))).astype(BF16)
            prev = d_gelu
            resid_mine, normed_two, gelu_out, d_up = {}, {}, {}, {}
            d_norm_two, part_two, y_mine = {}, {}, {}

            def norm_two_back(row0, prev):
                _, pull = jax.vjp(layer_norm, resid_mine[row0], gain_two.astype(F32))
                d_ln, d_gain = pull(after(d_norm_two[row0], prev))
                return mine(dy, row0) + d_ln, d_gain

            def y_share(row0, *prev):
                total = resid_mine[row0].astype(F32) + after(part_two[row0], *prev).astype(F32)
                y_mine[row0] = total.astype(BF16)
                return y_mine[row0]

            def down(row0, prev):
                part = mm(after(gelu_out[row0], prev), w_down, ((1,), (0,))).astype(BF16)
                part_two[row0] = scatter(part)
                return part

            for index, (row0, row1) in enumerate(order):
                resid, normed_two[row0] = proj_ln(after(attn_all[row0], prev), wo_all, x, gain_two, row0)
                resid_mine[row0] = lax.dynamic_slice_in_dim(resid, me * share, share, 0)
                up = mm(normed_two[row0], w_up, ((1,), (0,))).astype(BF16)
                gelu_out[row0], gelu_pull = jax.vjp(gelu_tanh, up)
                (d_up[row0],) = gelu_pull(d_gelu[row0:row1])
                prev = mm(d_up[row0], w_up, ((1,), (1,))).astype(BF16)
                d_norm_two[row0] = scatter(prev)
                if index < len(order) - 1:
                    prev = down(row0, prev)
            for row0, row1 in order[:-1]:
                prev = y_share(row0, prev)
            d_resid_mine, d_resid, d_gain_two = {}, {}, 0.0
            for index, (row0, row1) in enumerate(order):
                d_resid_mine[row0], d_gain = norm_two_back(row0, prev)
                d_gain_two = d_gain_two + d_gain
                prev = d_resid_mine[row0]
                d_resid[row0] = gather(prev)
                if index == 0:
                    joined_gelu = jnp.concatenate([gelu_out[r] for r, _ in order[::-1]], axis=0)
                    d_w_down = mm(after(joined_gelu, prev), dy, ((0,), (0,))).astype(BF16)
                    prev = d_w_down
            prev = down(order[-1][0], prev)
            y_all = {row0: gather(after(y_mine[row0], prev)) for row0, _ in order[:-1]}
            carry = None
            d_qkv, d_norm_one = {}, {}
            for row0, row1 in order:
                d_attn = mm(after(d_resid[row0], prev), wo, ((1,), (1,))).astype(BF16)
                result = attn_bwd(qkv, start_row, low, mid, d_attn, attn[row0], lse[row0], carry, n, d, row0, row1, blk)
                d_qkv[row0] = result[0]
                carry = result[1] if len(result) > 1 else None
                ready = list(y_all.values()) if row0 == order[-1][0] else []
                prev = mm(after(d_qkv[row0], *ready), w_qkv, ((1,), (1,))).astype(BF16)
                d_norm_one[row0] = scatter(prev)

            def summed(left, right):
                return sum(mm(left[row0], right[row0], ((0,), (0,))) for row0, _ in order)

            last = order[-1][0]
            y_all[last] = gather(y_share(last, prev))
            d_w_out = summed({r: after(v, prev) for r, v in attn.items()}, d_resid).astype(BF16)
            d_qkv_all = jnp.concatenate([d_qkv[row0] for row0, _ in order[::-1]], axis=0)
            d_w_qkv = mm(after(normed_one, d_w_out), d_qkv_all, ((0,), (0,))).astype(BF16)
            prev = d_w_qkv
            dx_all, d_gain_one = {}, 0.0
            for index, (row0, row1) in enumerate(order):
                _, pull = jax.vjp(layer_norm, mine(x, row0), gain_one.astype(F32))
                d_ln, d_gain = pull(after(d_norm_one[row0], prev))
                d_gain_one = d_gain_one + d_gain
                prev = d_resid_mine[row0] + d_ln
                dx_all[row0] = gather(prev)
                if index == 0:
                    d_w_up = summed({r: after(v, prev) for r, v in normed_two.items()}, d_up).astype(BF16)
                    prev = d_w_up
            d_gains = lax.psum(jnp.stack([d_gain_one, d_gain_two]), 'model')
            y_out, d_x = None, None
            for row0, _ in order:
                y_out = place(after(y_all[row0], prev), y_out, seq, row0)
                prev = y_out
            for row0, _ in order:
                d_x = place(after(dx_all[row0], prev), d_x, seq, row0)
                prev = d_x
            outs.append((y_out, d_x, d_w_qkv, d_w_out, d_w_up, d_w_down, d_gains))
        y_out = jnp.stack([out[0] for out in outs])
        d_x = jnp.stack([out[1] for out in outs])
        d_w_qkv, d_w_out, d_w_up, d_w_down, d_gains = (sum(out[k] for out in outs) for k in range(2, 7))
        d_gains = d_gains.astype(BF16)
        return (y_out, d_x, d_w_qkv.astype(BF16), d_w_out.astype(BF16).reshape(n, d, hidden), d_w_up.astype(BF16),
                d_w_down.astype(BF16), d_gains[0], d_gains[1])

    in_specs = (P('data'), P('data'), P(), P(None, 'model'), P('model'), P(), P(None, 'model'), P('model'), P('data'))
    out_specs = (P('data'), P('data'), P('data', 'model'), P(('data', 'model')), P('data', 'model'), P(('data', 'model')), P('data'), P('data'))
    return jax.shard_map(local_step, mesh=mesh, in_specs=in_specs, out_specs=out_specs, check_vma=False)
```

```python
import functools

import jax
import jax.numpy as jnp
from jax import lax
from jax.experimental import pallas as pl
from jax.experimental.pallas import tpu as pltpu
from jax.sharding import PartitionSpec as P

LN_EPS = 1e-5
LOG2E = 1.4426950408889634
MASKED = -1e30
N_CHUNKS = 2
VMEM_BYTES = 60 * 1024 * 1024
NT = (((1,), (1,)), ((), ()))
TN = (((0,), (0,)), ((), ()))
F32, BF16 = jnp.float32, jnp.bfloat16


def mm(a, b, dims):
    return lax.dot_general(a, b, (dims, ((), ())), preferred_element_type=F32)


def layer_norm(x_in, gain):
    x_wide = x_in.astype(F32)
    row_mean = jnp.mean(x_wide, axis=-1, keepdims=True)
    centered = x_wide - row_mean
    row_var = jnp.mean(centered * centered, axis=-1, keepdims=True)
    return (centered * lax.rsqrt(row_var + LN_EPS) * gain.astype(F32)).astype(BF16)


def gelu_tanh(up_proj):
    return jax.nn.gelu(up_proj.astype(F32), approximate=True).astype(BF16)


def after(value, *others):
    return lax.optimization_barrier((value, *others))[0]


def document_starts(seg):
    seq = seg.shape[0]
    side = 64
    before = jnp.concatenate([seg[:1], seg[:-1]])
    marks = jnp.where(seg != before, jnp.arange(seq, dtype=jnp.int32), 0).reshape(seq // side, side)
    upto = jnp.arange(side)[:, None] >= jnp.arange(side)[None, :]
    inside = jnp.max(jnp.where(upto[None], marks[:, None, :], 0), axis=-1)
    row = jnp.arange(seq // side)
    ahead = jnp.max(jnp.where(row[:, None] > row[None, :], jnp.max(marks, axis=-1)[None, :], 0), axis=-1)
    return jnp.maximum(inside, ahead[:, None]).reshape(seq)


def ln_qkv_kernel(x_ref, g_ref, w_ref, a_ref, qkv_ref):
    half = x_ref.shape[0] // 2
    for low in (0, half):
        normed = layer_norm(x_ref[low:low + half, :], g_ref[...])
        a_ref[low:low + half, :] = normed
        qkv_ref[low:low + half, :] = jnp.dot(normed, w_ref[...], preferred_element_type=F32).astype(BF16)


def ln_qkv(x, gain, w, rows=512):
    t, h = x.shape
    c = w.shape[1]
    return pl.pallas_call(
        ln_qkv_kernel,
        grid=(t // rows,),
        in_specs=[
            pl.BlockSpec((rows, h), lambda i: (i, 0)),
            pl.BlockSpec((1, h), lambda i: (0, 0)),
            pl.BlockSpec((h, c), lambda i: (0, 0)),
        ],
        out_specs=[pl.BlockSpec((rows, h), lambda i: (i, 0)), pl.BlockSpec((rows, c), lambda i: (i, 0))],
        out_shape=[jax.ShapeDtypeStruct((t, h), BF16), jax.ShapeDtypeStruct((t, c), BF16)],
        compiler_params=pltpu.CompilerParams(vmem_limit_bytes=VMEM_BYTES, dimension_semantics=('arbitrary',)),
        cost_estimate=pl.CostEstimate(flops=2 * t * h * c, bytes_accessed=4 * t * h + 2 * h * c + 2 * t * c, transcendentals=0),
        name='ln_qkv',
    )(x, gain.reshape(1, h), w)


def proj_ln_kernel(o_ref, w_ref, x_ref, g_ref, resid_ref, b_ref, o_scr):
    d = o_ref.shape[2]
    for r in range(o_ref.shape[0]):
        o_scr[:, r * d:(r + 1) * d] = o_ref[r]
    total = jnp.dot(o_scr[...], w_ref[...], preferred_element_type=F32)
    resid = (x_ref[...].astype(F32) + total).astype(BF16)
    resid_ref[...] = resid
    b_ref[...] = layer_norm(resid, g_ref[...])


def proj_ln(o_all, w_all, x, gain, row0, rows=256):
    n, t, d = o_all.shape
    h = x.shape[1]
    first = row0 // rows
    return pl.pallas_call(
        proj_ln_kernel,
        grid=(t // rows,),
        in_specs=[
            pl.BlockSpec((n, rows, d), lambda i: (0, i, 0)),
            pl.BlockSpec((n * d, h), lambda i: (0, 0), pipeline_mode=pl.Buffered(1)),
            pl.BlockSpec((rows, h), lambda i: (i + first, 0)),
            pl.BlockSpec((1, h), lambda i: (0, 0)),
        ],
        out_specs=[pl.BlockSpec((rows, h), lambda i: (i, 0))] * 2,
        scratch_shapes=[pltpu.VMEM((rows, n * d), BF16)],
        out_shape=[jax.ShapeDtypeStruct((t, h), BF16)] * 2,
        compiler_params=pltpu.CompilerParams(vmem_limit_bytes=VMEM_BYTES, dimension_semantics=('arbitrary',)),
        cost_estimate=pl.CostEstimate(flops=2 * t * n * d * h, bytes_accessed=2 * n * d * h + 8 * t * h, transcendentals=0),
        name='proj_ln',
    )(o_all, w_all, x, gain.reshape(1, h))


def place_kernel(part_ref, *refs):
    refs[-1][...] = part_ref[...]


def place(part, into, seq, row0, rows=256):
    t, h = part.shape
    first = row0 // rows
    in_specs = [pl.BlockSpec((rows, h), lambda i: (i, 0))]
    if into is not None:
        in_specs.append(pl.BlockSpec(memory_space=pl.ANY))
    return pl.pallas_call(
        place_kernel,
        grid=(t // rows,),
        in_specs=in_specs,
        out_specs=pl.BlockSpec((rows, h), lambda i: (i + first, 0)),
        out_shape=jax.ShapeDtypeStruct((seq, h), part.dtype),
        input_output_aliases={} if into is None else {1: 0},
        compiler_params=pltpu.CompilerParams(vmem_limit_bytes=VMEM_BYTES, dimension_semantics=('arbitrary',)),
        cost_estimate=pl.CostEstimate(flops=16 * t * h, bytes_accessed=4 * t * h, transcendentals=0),
        name='place',
    )(part, *(() if into is None else (into,)))


def split_kv(qkv_ref, k_scr, v_scr, blk):
    n, rows, d = k_scr.shape

    def body(j, carry):
        at = pl.ds(pl.multiple_of(j * blk, blk), blk)
        for h in range(n):
            k_scr[h, at, :] = qkv_ref[at, (3 * h + 1) * d:(3 * h + 2) * d]
            v_scr[h, at, :] = qkv_ref[at, (3 * h + 2) * d:(3 * h + 3) * d]
        return carry

    lax.fori_loop(0, rows // blk, body, 0)


def attn_fwd_kernel(first, low_ref, mid_ref, q_ref, kv_ref, start_ref, o_ref, lse_ref, k_scr, v_scr, m_scr, l_scr, acc_scr):
    step = pl.program_id(0)
    n, _, d = k_scr.shape
    blk = q_ref.shape[0]
    scale = d ** -0.5 * LOG2E

    @pl.when(step == 0)
    def _():
        split_kv(kv_ref, k_scr, v_scr, blk)

    i = step + first
    queries = [q_ref[:, 3 * h * d:(3 * h + 1) * d] for h in range(n)]
    start = start_ref[...]
    m_scr[...] = jnp.full(m_scr.shape, MASKED, F32)
    l_scr[...] = jnp.zeros(l_scr.shape, F32)
    acc_scr[...] = jnp.zeros(acc_scr.shape, F32)

    def block(j, kind):
        at = pl.ds(pl.multiple_of(j * blk, blk), blk)
        if kind != 'full':
            keys = j * blk + lax.broadcasted_iota(jnp.int32, (blk, blk), 0)
            seen = keys >= start
            if kind == 'diagonal':
                seen = seen & (keys <= i * blk + lax.broadcasted_iota(jnp.int32, (blk, blk), 1))
        for h in range(n):
            s = lax.dot_general(k_scr[h, at, :], queries[h], NT, preferred_element_type=F32) * scale
            if kind != 'full':
                s = jnp.where(seen, s, MASKED)
            m_old = m_scr[h:h + 1, :]
            m_new = jnp.maximum(m_old, jnp.max(s, axis=0, keepdims=True))
            p = jnp.exp2(s - m_new)
            alpha = jnp.exp2(m_old - m_new)
            l_scr[h:h + 1, :] = l_scr[h:h + 1, :] * alpha + jnp.sum(p, axis=0, keepdims=True)
            m_scr[h:h + 1, :] = m_new
            acc_scr[h] = acc_scr[h] * alpha + lax.dot_general(v_scr[h, at, :], p.astype(BF16), TN, preferred_element_type=F32)

    low = low_ref[i]
    mid = jnp.minimum(mid_ref[i], i)
    pl.loop(low, mid)(lambda j: block(j, 'masked'))
    pl.loop(mid, i)(lambda j: block(j, 'full'))
    block(i, 'diagonal')
    for h in range(n):
        o_ref[:, h * d:(h + 1) * d] = jnp.transpose(acc_scr[h] / l_scr[h:h + 1, :]).astype(BF16)
    lse_ref[...] = jnp.where(l_scr[...] > 0, m_scr[...] + jnp.log2(jnp.maximum(l_scr[...], 1e-30)), 0.0)


def attn_fwd(qkv, start, low, mid, n, d, row0, row1, blk):
    rows = row1 - row0
    c = qkv.shape[1]
    first = row0 // blk
    pairs = n * (row1 * row1 - row0 * row0) // 2
    return pl.pallas_call(
        functools.partial(attn_fwd_kernel, first),
        grid_spec=pltpu.PrefetchScalarGridSpec(
            num_scalar_prefetch=2,
            grid=(rows // blk,),
            in_specs=[
                pl.BlockSpec((blk, c), lambda i, *_: (i + first, 0)),
                pl.BlockSpec((row1, c), lambda i, *_: (0, 0), pipeline_mode=pl.Buffered(1)),
                pl.BlockSpec((1, blk), lambda i, *_: (0, i + first)),
            ],
            out_specs=[pl.BlockSpec((blk, n * d), lambda i, *_: (i, 0)), pl.BlockSpec((8, blk), lambda i, *_: (0, i))],
            scratch_shapes=[
                pltpu.VMEM((n, row1, d), BF16),
                pltpu.VMEM((n, row1, d), BF16),
                pltpu.VMEM((8, blk), F32),
                pltpu.VMEM((8, blk), F32),
                pltpu.VMEM((n, d, blk), F32),
            ],
        ),
        out_shape=[jax.ShapeDtypeStruct((rows, n * d), BF16), jax.ShapeDtypeStruct((8, rows), F32)],
        compiler_params=pltpu.CompilerParams(vmem_limit_bytes=VMEM_BYTES, dimension_semantics=('arbitrary',)),
        cost_estimate=pl.CostEstimate(flops=2 * 4 * pairs * d, bytes_accessed=2 * row1 * c + 2 * rows * n * d, transcendentals=pairs),
        name='attn_fwd',
    )(low, mid, qkv, qkv, start)


def attn_bwd_kernel(last, final, low_ref, mid_ref, q_ref, kv_ref, start_ref, do_ref, o_ref, lse_ref, *rest):
    if final:
        carry_ref, out_ref, k_scr, v_scr, acc_scr, dq_scr, stat_scr, sem = rest
    else:
        out_ref, carry_ref, k_scr, v_scr, acc_scr, dq_scr, stat_scr, sem = rest
    step = pl.program_id(0)
    n, _, d = k_scr.shape
    blk = q_ref.shape[0]
    scale = d ** -0.5

    @pl.when(step == 0)
    def _():
        split_kv(kv_ref, k_scr, v_scr, blk)
        if final:
            copy = pltpu.make_async_copy(carry_ref, acc_scr, sem)
            copy.start()
            copy.wait()
        else:
            def clear(j, carry):
                at = pl.ds(pl.multiple_of(j * blk, blk), blk)
                for h in range(2 * n):
                    acc_scr[h, at, :] = jnp.zeros((blk, d), F32)
                return carry
            lax.fori_loop(0, acc_scr.shape[1] // blk, clear, 0)

    i = last - step
    queries = [q_ref[:, 3 * h * d:(3 * h + 1) * d] for h in range(n)]
    d_outs = [do_ref[:, h * d:(h + 1) * d] for h in range(n)]
    start = start_ref[...]
    lanes = lax.broadcasted_iota(jnp.int32, (blk, 128), 1)
    delta = jnp.zeros((blk, 128), F32)
    for h in range(n):
        prod = d_outs[h].astype(F32) * o_ref[:, h * d:(h + 1) * d].astype(F32)
        delta = jnp.where(lanes == h, jnp.sum(prod, axis=-1, keepdims=True), delta)
    stat_scr[0] = lse_ref[...]
    stat_scr[1] = jnp.transpose(delta)[:8]
    dq_scr[...] = jnp.zeros(dq_scr.shape, F32)

    def block(j, kind):
        at = pl.ds(pl.multiple_of(j * blk, blk), blk)
        if kind != 'full':
            keys = j * blk + lax.broadcasted_iota(jnp.int32, (blk, blk), 0)
            seen = keys >= start
            if kind == 'diagonal':
                seen = seen & (keys <= i * blk + lax.broadcasted_iota(jnp.int32, (blk, blk), 1))
        for h in range(n):
            k = k_scr[h, at, :]
            s = lax.dot_general(k, queries[h], NT, preferred_element_type=F32) * (scale * LOG2E)
            if kind != 'full':
                s = jnp.where(seen, s, MASKED)
            p = jnp.exp2(s - stat_scr[0, h:h + 1, :])
            dp = lax.dot_general(v_scr[h, at, :], d_outs[h], NT, preferred_element_type=F32)
            ds = (p * (dp - stat_scr[1, h:h + 1, :])).astype(BF16)
            acc_scr[n + h, at, :] += jnp.dot(p.astype(BF16), d_outs[h], preferred_element_type=F32)
            acc_scr[h, at, :] += jnp.dot(ds, queries[h], preferred_element_type=F32)
            dq_scr[h] += lax.dot_general(ds, k, TN, preferred_element_type=F32)

    low = low_ref[i]
    mid = jnp.minimum(mid_ref[i], i)
    pl.loop(low, mid)(lambda j: block(j, 'masked'))
    pl.loop(mid, i)(lambda j: block(j, 'full'))
    block(i, 'diagonal')
    at = pl.ds(pl.multiple_of(i * blk, blk), blk)
    for h in range(n):
        out_ref[:, 3 * h * d:(3 * h + 1) * d] = (dq_scr[h] * scale).astype(BF16)
        out_ref[:, (3 * h + 1) * d:(3 * h + 2) * d] = (acc_scr[h, at, :] * scale).astype(BF16)
        out_ref[:, (3 * h + 2) * d:(3 * h + 3) * d] = acc_scr[n + h, at, :].astype(BF16)

    if not final:
        @pl.when(step == pl.num_programs(0) - 1)
        def _():
            copy = pltpu.make_async_copy(acc_scr.at[:, 0:carry_ref.shape[1], :], carry_ref, sem)
            copy.start()
            copy.wait()


def attn_bwd(qkv, start_row, low, mid, d_out, o, lse, carry, n, d, row0, row1, blk):
    rows = row1 - row0
    c = qkv.shape[1]
    count = rows // blk
    last = row1 // blk - 1
    final = row0 == 0
    pairs = n * (row1 * row1 - row0 * row0) // 2
    out_shape = [jax.ShapeDtypeStruct((rows, c), BF16)]
    out_specs = [pl.BlockSpec((blk, c), lambda i, *_: (count - 1 - i, 0))]
    in_specs = [
        pl.BlockSpec((blk, c), lambda i, *_: (last - i, 0)),
        pl.BlockSpec((row1, c), lambda i, *_: (0, 0), pipeline_mode=pl.Buffered(1)),
        pl.BlockSpec((1, blk), lambda i, *_: (0, last - i)),
        pl.BlockSpec((blk, n * d), lambda i, *_: (count - 1 - i, 0)),
        pl.BlockSpec((blk, n * d), lambda i, *_: (count - 1 - i, 0)),
        pl.BlockSpec((8, blk), lambda i, *_: (0, count - 1 - i)),
    ]
    args = [low, mid, qkv, qkv, start_row, d_out, o, lse]
    assert final == (carry is not None) or row1 == qkv.shape[0]
    if final:
        if carry is None:
            carry = jnp.zeros((2 * n, row1, d), F32)
        in_specs.append(pl.BlockSpec(memory_space=pl.ANY))
        args.append(carry)
    else:
        out_shape.append(jax.ShapeDtypeStruct((2 * n, row0, d), F32))
        out_specs.append(pl.BlockSpec(memory_space=pl.ANY))
    return pl.pallas_call(
        functools.partial(attn_bwd_kernel, last, final),
        grid_spec=pltpu.PrefetchScalarGridSpec(
            num_scalar_prefetch=2,
            grid=(count,),
            in_specs=in_specs,
            out_specs=out_specs,
            scratch_shapes=[
                pltpu.VMEM((n, row1, d), BF16),
                pltpu.VMEM((n, row1, d), BF16),
                pltpu.VMEM((2 * n, row1, d), F32),
                pltpu.VMEM((n, blk, d), F32),
                pltpu.VMEM((2, 8, blk), F32),
                pltpu.SemaphoreType.DMA,
            ],
        ),
        out_shape=out_shape,
        compiler_params=pltpu.CompilerParams(vmem_limit_bytes=VMEM_BYTES, dimension_semantics=('arbitrary',)),
        cost_estimate=pl.CostEstimate(flops=2 * 10 * pairs * d, bytes_accessed=4 * row1 * c + 4 * rows * n * d, transcendentals=pairs),
        name='attn_bwd',
    )(*args)


def solution(mesh):
    def local_step(x_in, seg_ids, gain_one, w_qkv, w_out, gain_two, w_up, w_down, d_y):
        rows, seq, hidden = x_in.shape
        n, d = w_out.shape[:2]
        blk = min(512, seq)
        size = seq // N_CHUNKS
        order = [(c * size, (c + 1) * size) for c in range(N_CHUNKS)][::-1]
        me = lax.axis_index('model')
        share = size // mesh.shape['model']

        def mine(full, row0):
            return lax.dynamic_slice_in_dim(full, row0 + me * share, share, 0)

        def gather(part):
            return lax.all_gather(part, 'model', axis=0, tiled=True)

        def scatter(part):
            return lax.psum_scatter(part, 'model', scatter_dimension=0, tiled=True)

        outs = []
        for b in range(rows):
            x, dy, seg = x_in[b], d_y[b], seg_ids[b]
            start = document_starts(seg)
            low = start[::blk] // blk
            mid = (start[blk - 1::blk] + blk - 1) // blk
            start_row = start.reshape(1, seq)

            wo = w_out.reshape(n * d, hidden)
            wo_all = gather(wo)
            normed_one, qkv = ln_qkv(x, gain_one, w_qkv)
            attn, lse, attn_all = {}, {}, {}
            prev = ()
            for row0, row1 in order:
                attn[row0], lse[row0] = attn_fwd(after(qkv, *prev), start_row, low, mid, n, d, row0, row1, blk)
                attn_all[row0] = lax.all_gather(attn[row0], 'model', axis=0, tiled=False)
                prev = (attn[row0], wo_all)
            d_gelu = mm(after(dy, *prev), w_down, ((1,), (1,))).astype(BF16)
            prev = d_gelu
            resid_mine, normed_two, gelu_out, d_up = {}, {}, {}, {}
            d_norm_two, part_two, y_mine = {}, {}, {}

            def norm_two_back(row0, prev):
                _, pull = jax.vjp(layer_norm, resid_mine[row0], gain_two.astype(F32))
                d_ln, d_gain = pull(after(d_norm_two[row0], prev))
                return mine(dy, row0) + d_ln, d_gain

            def y_share(row0, *prev):
                total = resid_mine[row0].astype(F32) + after(part_two[row0], *prev).astype(F32)
                y_mine[row0] = total.astype(BF16)
                return y_mine[row0]

            def down(row0, *prev):
                part = mm(after(gelu_out[row0], *prev), w_down, ((1,), (0,))).astype(BF16)
                part_two[row0] = scatter(part)
                return part

            for index, (row0, row1) in enumerate(order):
                resid, normed_two[row0] = proj_ln(after(attn_all[row0], prev), wo_all, x, gain_two, row0)
                resid_mine[row0] = lax.dynamic_slice_in_dim(resid, me * share, share, 0)
                up = mm(normed_two[row0], w_up, ((1,), (0,))).astype(BF16)
                gelu_out[row0], gelu_pull = jax.vjp(gelu_tanh, up)
                (d_up[row0],) = gelu_pull(d_gelu[row0:row1])
                gelu_out[row0], d_up[row0] = lax.optimization_barrier((gelu_out[row0], d_up[row0]))
                prev = mm(d_up[row0], w_up, ((1,), (1,))).astype(BF16)
                d_norm_two[row0] = scatter(prev)
                if index < len(order) - 1:
                    prev = down(row0)
            for row0, row1 in order[:-1]:
                prev = y_share(row0, prev)
            d_resid_mine, d_resid, d_gain_two = {}, {}, 0.0
            for index, (row0, row1) in enumerate(order):
                d_resid_mine[row0], d_gain = norm_two_back(row0, prev)
                d_gain_two = d_gain_two + d_gain
                prev = d_resid_mine[row0]
                d_resid[row0] = gather(prev)
                if index == 0:
                    joined_gelu = jnp.concatenate([gelu_out[r] for r, _ in order[::-1]], axis=0)
                    d_w_down = mm(after(joined_gelu, prev), dy, ((0,), (0,))).astype(BF16)
                    prev = d_w_down
            prev = down(order[-1][0], prev)
            y_all = {row0: gather(after(y_mine[row0], prev)) for row0, _ in order[:-1]}
            carry = None
            d_qkv, d_norm_one = {}, {}
            for row0, row1 in order:
                d_attn = mm(after(d_resid[row0], prev), wo, ((1,), (1,))).astype(BF16)
                result = attn_bwd(qkv, start_row, low, mid, d_attn, attn[row0], lse[row0], carry, n, d, row0, row1, blk)
                d_qkv[row0] = result[0]
                carry = result[1] if len(result) > 1 else None
                ready = list(y_all.values()) if row0 == order[-1][0] else []
                prev = mm(after(d_qkv[row0], *ready), w_qkv, ((1,), (1,))).astype(BF16)
                d_norm_one[row0] = scatter(prev)

            def summed(left, right):
                return sum(mm(left[row0], right[row0], ((0,), (0,))) for row0, _ in order)

            last = order[-1][0]
            y_all[last] = gather(y_share(last, prev))
            d_w_out = summed({r: after(v, prev) for r, v in attn.items()}, d_resid).astype(BF16)
            d_qkv_all = jnp.concatenate([d_qkv[row0] for row0, _ in order[::-1]], axis=0)
            d_w_qkv = mm(after(normed_one, d_w_out), d_qkv_all, ((0,), (0,))).astype(BF16)
            prev = d_w_qkv
            dx_all, d_gain_one = {}, 0.0
            for index, (row0, row1) in enumerate(order):
                _, pull = jax.vjp(layer_norm, mine(x, row0), gain_one.astype(F32))
                d_ln, d_gain = pull(after(d_norm_one[row0], prev))
                d_gain_one = d_gain_one + d_gain
                prev = d_resid_mine[row0] + d_ln
                dx_all[row0] = gather(prev)
                if index == 0:
                    d_w_up = summed({r: after(v, prev) for r, v in normed_two.items()}, d_up).astype(BF16)
                    prev = d_w_up
            d_gains = lax.psum(jnp.stack([d_gain_one, d_gain_two]), 'model')
            y_out, d_x = None, None
            for row0, _ in order:
                y_out = place(after(y_all[row0], prev), y_out, seq, row0)
                prev = y_out
            for row0, _ in order:
                d_x = place(after(dx_all[row0], prev), d_x, seq, row0)
                prev = d_x
            outs.append((y_out, d_x, d_w_qkv, d_w_out, d_w_up, d_w_down, d_gains))
        y_out = jnp.stack([out[0] for out in outs])
        d_x = jnp.stack([out[1] for out in outs])
        d_w_qkv, d_w_out, d_w_up, d_w_down, d_gains = (sum(out[k] for out in outs) for k in range(2, 7))
        d_gains = d_gains.astype(BF16)
        return (y_out, d_x, d_w_qkv.astype(BF16), d_w_out.astype(BF16).reshape(n, d, hidden), d_w_up.astype(BF16),
                d_w_down.astype(BF16), d_gains[0], d_gains[1])

    in_specs = (P('data'), P('data'), P(), P(None, 'model'), P('model'), P(), P(None, 'model'), P('model'), P('data'))
    out_specs = (P('data'), P('data'), P('data', 'model'), P(('data', 'model')), P('data', 'model'), P(('data', 'model')), P('data'), P('data'))
    return jax.shard_map(local_step, mesh=mesh, in_specs=in_specs, out_specs=out_specs, check_vma=False)
```
